32 devices in a mesh: lat: 2 (over core), lon: 2 (over y), lev: 2 (over x), unit: 4 (over z).
Axes of the slice: x: 2, y: 2, z: 4, core: 2. Of those that a mesh axis runs over, the one named last changes fastest.
Arguments:
- tracer: float32 [32, 256, 32, 128], P(('unit', 'lat'), 'lon', 'lev'), parts along dimension 0, may hold values from 0.5 to 2
- diffusivity: float32 [32, 256, 32, 128], P(('unit', 'lat'), 'lon', 'lev'), parts along dimension 0, may hold values from 0.03 to 0.15
- source: float32 [32, 256, 32, 128], P(('unit', 'lat'), 'lon', 'lev'), parts along dimension 0, may hold values from -0.2 to 0.2
Outputs:
- standardized: float32 [32, 256, 32, 128], P(('unit', 'lat'), 'lon', 'lev'), parts along dimension 0
- tracer_end: float32 [32, 256, 32, 128], P(('unit', 'lat'), 'lon', 'lev'), parts along dimension 0
The draws below stay inside these ranges and needn't reach their ends.
There are 4 independent parts, one for each index of `unit`. The reference program is written for one: setup_inputs(seed, part) draws one part's arguments, and reference() takes and returns one part's arrays. A program takes and returns all parts, laid end to end along the dimension named above; each array names one. Nothing has to cross between parts.
All inputs are finite; a program needn't handle non-finite values.
Results may differ from the reference program's by a relative error of at most 0.00002.
Values sent between devices are 32-bit elements; how exact they have to be, the bound alone decides.
A program may use at most 128 MiB of HBM per device.

```python
import jax
import jax.numpy as jnp
from jax import lax

GRID_J = 8
GRID_I = 256
GRID_K = 32
LEVELS = 128
STEPS = 4


def steps_of(rng, extent, split, smallest, largest):
    gain = 1.0
    for dim, parts in split:
        steps = jax.random.uniform(jax.random.fold_in(jax.random.fold_in(rng, 6), dim), (parts,), jnp.float32, smallest / len(split), largest / len(split))
        gain = gain * jnp.repeat(jnp.exp(steps), extent[dim] // parts).reshape((-1,) + (1,) * (len(extent) - 1 - dim))
    return gain


def setup_inputs(seed: int = 0, part: int = 0) -> dict:
    streams_of = jax.random.split(jax.random.key(seed), 4)
    part_keys = jax.random.split(jax.random.fold_in(streams_of[3], part), 4)
    return {
        "tracer": jnp.clip(0.5 + 1.5 * jax.random.uniform(part_keys[0], (GRID_J, GRID_I, GRID_K, LEVELS), jnp.float32) ** steps_of(part_keys[0], (GRID_J, GRID_I, GRID_K, LEVELS), ((0, 2), (1, 2), (2, 2)), -0.2, 0.2), 0.5, 2.0),
        "diffusivity": jnp.clip(0.03 + 0.120000007 * jax.random.uniform(part_keys[1], (GRID_J, GRID_I, GRID_K, LEVELS), jnp.float32) ** steps_of(part_keys[1], (GRID_J, GRID_I, GRID_K, LEVELS), ((0, 2), (1, 2), (2, 2)), -0.2, 0.2), 0.03, 0.15),
        "source": jnp.clip(jax.random.uniform(part_keys[2], (GRID_J, GRID_I, GRID_K, LEVELS), jnp.float32, -0.2, 0.2) * steps_of(part_keys[2], (GRID_J, GRID_I, GRID_K, LEVELS), ((0, 2), (1, 2), (2, 2)), -0.4, 0.0), -0.2, 0.2),
    }


def strip_edges(values, dims):
    for dim in dims:
        values = lax.slice_in_dim(values, 1, values.shape[dim] - 1, axis=dim)
    return values

def neighbour(values, dim, start, dims):
    others = [other for other in dims if other != dim]
    values = strip_edges(values, others)
    return lax.slice_in_dim(values, start, start + values.shape[dim] - 2, axis=dim)

def one_step(padded, diffusivity, source):
    middle = strip_edges(padded, (0, 1, 2))
    lower = [neighbour(padded, dim, 0, (0, 1, 2)) for dim in (0, 1, 2)]
    upper = [neighbour(padded, dim, 2, (0, 1, 2)) for dim in (0, 1, 2)]
    spread = lower[0] + upper[0] + lower[1] + upper[1] + lower[2] + upper[2] - 6.0 * middle
    return middle + diffusivity * spread + source

def reference(tracer, diffusivity, source):
    for step in range(STEPS):
        tracer = one_step(jnp.pad(tracer, ((1, 1), (1, 1), (1, 1), (0, 0)), mode='wrap'), diffusivity, source)
    line_mean = lax.optimization_barrier(jnp.mean(tracer, axis=2, keepdims=True))
    centred = tracer - line_mean
    line_variance = lax.optimization_barrier(jnp.mean(centred * centred, axis=2, keepdims=True))
    standardized = centred * lax.rsqrt(line_variance + 0.0001)
    return (standardized, tracer)
```

```python
import functools

import jax
import jax.numpy as jnp
from jax import lax
from jax.experimental import pallas as pl
from jax.experimental.pallas import tpu as pltpu
from jax.sharding import PartitionSpec as P

STEPS = 4
PAD = 8
EPSILON = 0.0001
MESH = pl.DeviceIdType.MESH


def rows_of(extent):
    for rows in (32, 16, 8):
        if extent % rows == 0:
            return rows
    return extent


def steps_kernel(
    sizes, shape, tracer, diffusivity, source, last, stats,
    field, coeff, forcing, own, others,
    load_sem, lev_send, lev_recv, lat_send, lat_recv, lon_send, lon_recv, stat_send, stat_recv,
):
    n_j, n_i, n_k, _ = shape
    n_lat, n_lon, n_lev = sizes
    inner = pl.ds(PAD, n_i)
    whole_j = pl.ds(1, n_j)
    chunk = rows_of(n_i)
    lat, lon, lev = lax.axis_index("lat"), lax.axis_index("lon"), lax.axis_index("lev")
    lat_up, lat_down = lax.rem(lat + 1, n_lat), lax.rem(lat + n_lat - 1, n_lat)
    lon_up, lon_down = lax.rem(lon + 1, n_lon), lax.rem(lon + n_lon - 1, n_lon)
    lev_up, lev_down = lax.rem(lev + 1, n_lev), lax.rem(lev + n_lev - 1, n_lev)

    def load(which, k):
        array = (tracer, diffusivity, source)[which]
        if which == 0:
            target = field.at[0, k + 1, whole_j, inner, :]
        else:
            target = (coeff, forcing)[which - 1].at[k]
        return pltpu.make_async_copy(array.at[:, :, k, :], target, load_sem.at[which, k])

    def remote(src, dst, send, recv, device):
        return pltpu.make_async_remote_copy(
            src_ref=src, dst_ref=dst, send_sem=send, recv_sem=recv,
            device_id=device, device_id_type=MESH,
        )

    def lev_copies(step, j):
        down = remote(
            field.at[step, 1, j, inner, :], field.at[step, n_k + 1, j, inner, :],
            lev_send.at[step, j - 1, 0], lev_recv.at[step, j - 1, 0], {"lev": lev_down},
        )
        up = remote(
            field.at[step, n_k, j, inner, :], field.at[step, 0, j, inner, :],
            lev_send.at[step, j - 1, 1], lev_recv.at[step, j - 1, 1], {"lev": lev_up},
        )
        return down, up

    parts = (pl.ds(1, 1), pl.ds(n_k, 1), pl.ds(2, n_k - 2))

    def lat_copy(step, part, side):
        k = parts[part]
        src, dst, to = ((1, n_j + 1, lat_down), (n_j, 0, lat_up))[side]
        return remote(
            field.at[step, k, src, inner, :], field.at[step, k, dst, inner, :],
            lat_send.at[step, part, side], lat_recv.at[step, part, side], {"lat": to},
        )

    def lon_copy(step, part, side):
        k = parts[part]
        src, dst, to = (
            (PAD, PAD + n_i, lon_down), (PAD + n_i - 1, PAD - 1, lon_up)
        )[side]
        return remote(
            field.at[step, k, whole_j, pl.ds(src, 1), :],
            field.at[step, k, whole_j, pl.ds(dst, 1), :],
            lon_send.at[step, part, side], lon_recv.at[step, part, side], {"lon": to},
        )

    def stat_copies(j):
        return [
            remote(
                own.at[j - 1], others.at[n_lev - 1 - away, j - 1],
                stat_send.at[away - 1, j - 1], stat_recv.at[n_lev - 1 - away, j - 1],
                {"lev": lax.rem(lev + away, n_lev)},
            )
            for away in range(1, n_lev)
        ]

    def update(step, k, j):
        for low in range(0, n_i, chunk):
            r = PAD + low
            middle = field[step, k, j, pl.ds(r, chunk), :]
            spread = (
                field[step, k, j - 1, pl.ds(r, chunk), :] + field[step, k, j + 1, pl.ds(r, chunk), :]
                + field[step, k, j, pl.ds(r - 1, chunk), :] + field[step, k, j, pl.ds(r + 1, chunk), :]
                + field[step, k - 1, j, pl.ds(r, chunk), :] + field[step, k + 1, j, pl.ds(r, chunk), :]
                - 6.0 * middle
            )
            rows = pl.ds(low, chunk)
            value = middle + coeff[k - 1, j - 1, rows, :] * spread + forcing[k - 1, j - 1, rows, :]
            if step == STEPS - 1:
                last[k - 1, j - 1, rows, :] = value
            else:
                field[step + 1, k, j, pl.ds(r, chunk), :] = value

    def summarise(j):
        for low in range(0, n_i, chunk):
            rows = pl.ds(low, chunk)
            total = last[0, j - 1, rows, :]
            for k in range(1, n_k):
                total = total + last[k, j - 1, rows, :]
            mean = total * (1.0 / n_k)
            squares = jnp.zeros_like(mean)
            for k in range(n_k):
                moved = last[k, j - 1, rows, :] - mean
                squares = squares + moved * moved
            own[j - 1, 0, rows, :] = mean
            own[j - 1, 1, rows, :] = squares

    def combine(j):
        for low in range(0, n_i, chunk):
            rows = pl.ds(low, chunk)
            means = [own[j - 1, 0, rows, :]] + [others[p, j - 1, 0, rows, :] for p in range(n_lev - 1)]
            mean = functools.reduce(jnp.add, means) * (1.0 / n_lev)
            squares = own[j - 1, 1, rows, :]
            for p in range(n_lev - 1):
                squares = squares + others[p, j - 1, 1, rows, :]
            for part in means:
                squares = squares + n_k * ((part - mean) * (part - mean))
            stats[j - 1, 0, rows, :] = mean
            stats[j - 1, 1, rows, :] = lax.rsqrt(squares * (1.0 / (n_k * n_lev)) + EPSILON)

    def over_k(first, end, body):
        def wrapped(k, carry):
            body(k)
            return carry
        lax.fori_loop(first, end, wrapped, 0)

    edges = (0, n_k - 1)
    for k in (0, n_k - 1, 1, n_k - 2):
        load(0, k).start()
    for which in (1, 2):
        for k in edges:
            load(which, k).start()
    over_k(2, n_k - 2, lambda k: load(0, k).start())
    for which in (1, 2):
        over_k(1, n_k - 1, lambda k: load(which, k).start())

    barrier = pltpu.get_barrier_semaphore()
    greeted = (
        [{"lat": lax.rem(lat + a, n_lat)} for a in sorted({1, n_lat - 1})]
        + [{"lon": lax.rem(lon + a, n_lon)} for a in sorted({1, n_lon - 1})]
        + [{"lev": lax.rem(lev + a, n_lev)} for a in range(1, n_lev)]
    )
    for device in greeted:
        pl.semaphore_signal(barrier, inc=1, device_id=device, device_id_type=MESH)
    pl.semaphore_wait(barrier, len(greeted))

    for k in edges:
        load(0, k).wait()
    for j in range(1, n_j + 1):
        for copy in lev_copies(0, j):
            copy.start()
    for part in (0, 1):
        for side in (0, 1):
            lat_copy(0, part, side).start()
            lon_copy(0, part, side).start()
    for k in (1, n_k - 2):
        load(0, k).wait()
    for which in (1, 2):
        for k in edges:
            load(which, k).wait()

    def inside(step):
        for side in (0, 1):
            lat_copy(step, 2, side).wait_recv()
            lon_copy(step, 2, side).wait_recv()

        def body(k):
            def across(j, carry):
                update(step, k, j)
                return carry
            lax.fori_loop(1, n_j + 1, across, 0)

        over_k(2, n_k, body)
        if step < STEPS - 1:
            for side in (0, 1):
                lat_copy(step + 1, 2, side).start()
                lon_copy(step + 1, 2, side).start()

    def outside(step):
        for part in (0, 1):
            for side in (0, 1):
                lat_copy(step, part, side).wait_recv()
                lon_copy(step, part, side).wait_recv()
        for j in range(1, n_j + 1):
            for copy in lev_copies(step, j):
                copy.wait_recv()
            update(step, 1, j)
            update(step, n_k, j)
            if step < STEPS - 1:
                for copy in lev_copies(step + 1, j):
                    copy.start()
                for side, edge in ((0, 1), (1, n_j)):
                    if j == edge:
                        for part in (0, 1):
                            lat_copy(step + 1, part, side).start()
            else:
                summarise(j)
                for copy in stat_copies(j):
                    copy.start()
        if step < STEPS - 1:
            for part in (0, 1):
                for side in (0, 1):
                    lon_copy(step + 1, part, side).start()

    over_k(2, n_k - 2, lambda k: load(0, k).wait())
    for side in (0, 1):
        lat_copy(0, 2, side).start()
        lon_copy(0, 2, side).start()
    outside(0)
    for which in (1, 2):
        over_k(1, n_k - 1, lambda k: load(which, k).wait())
    inside(0)
    for step in range(1, STEPS):
        inside(step)
        outside(step)
    for j in range(1, n_j + 1):
        for copy in stat_copies(j):
            copy.wait_recv()
        combine(j)

    for step in range(STEPS):
        for j in range(1, n_j + 1):
            for copy in lev_copies(step, j):
                copy.wait_send()
        for part in range(3):
            for side in (0, 1):
                lat_copy(step, part, side).wait_send()
                lon_copy(step, part, side).wait_send()
    for j in range(1, n_j + 1):
        for copy in stat_copies(j):
            copy.wait_send()


def finish_kernel(n_k, rows, last, stats, standardized, tracer_end):
    j, block = pl.program_id(0), pl.program_id(1)
    for low in range(0, rows, 8):
        here = pl.ds(pl.multiple_of(block * rows + low, 8), 8)
        mean = stats[j, 0, here, :]
        scale = stats[j, 1, here, :]
        for k in range(n_k):
            value = last[k, j, here, :]
            place = pl.ds(low * n_k + k, 8, stride=n_k)
            tracer_end[0, place, :] = value
            standardized[0, place, :] = (value - mean) * scale


def on_device(sizes, tracer, diffusivity, source):
    shape = tracer.shape
    n_j, n_i, n_k, levels = shape
    n_lev = sizes[2]
    f32 = jnp.float32
    sem = pltpu.SemaphoreType.DMA
    last, stats = pl.pallas_call(
        functools.partial(steps_kernel, sizes, shape),
        out_shape=(
            pltpu.VMEM((n_k, n_j, n_i, levels), f32),
            pltpu.VMEM((n_j, 2, n_i, levels), f32),
        ),
        in_specs=[pl.BlockSpec(memory_space=pl.ANY)] * 3,
        out_specs=(pl.BlockSpec(memory_space=pltpu.VMEM),) * 2,
        scratch_shapes=[
            pltpu.VMEM((STEPS, n_k + 2, n_j + 2, n_i + 2 * PAD, levels), f32),
            pltpu.VMEM((n_k, n_j, n_i, levels), f32),
            pltpu.VMEM((n_k, n_j, n_i, levels), f32),
            pltpu.VMEM((n_j, 2, n_i, levels), f32),
            pltpu.VMEM((n_lev - 1, n_j, 2, n_i, levels), f32),
            sem((3, n_k)),
            sem((STEPS, n_j, 2)), sem((STEPS, n_j, 2)),
            sem((STEPS, 3, 2)), sem((STEPS, 3, 2)),
            sem((STEPS, 3, 2)), sem((STEPS, 3, 2)),
            sem((n_lev - 1, n_j)), sem((n_lev - 1, n_j)),
        ],
        compiler_params=pltpu.CompilerParams(
            collective_id=0, has_side_effects=True, vmem_limit_bytes=48 * 1024 * 1024,
        ),
    )(tracer, diffusivity, source)
    rows = rows_of(n_i)
    block = pl.BlockSpec((1, rows * n_k, levels), lambda j, i: (j, i, 0))
    whole = pl.BlockSpec(memory_space=pltpu.VMEM)
    flat = jax.ShapeDtypeStruct((n_j, n_i * n_k, levels), f32)
    standardized, tracer_end = pl.pallas_call(
        functools.partial(finish_kernel, n_k, rows),
        grid=(n_j, n_i // rows),
        out_shape=(flat, flat),
        in_specs=[whole, whole],
        out_specs=(block, block),
        compiler_params=pltpu.CompilerParams(vmem_limit_bytes=24 * 1024 * 1024),
    )(last, stats)
    return standardized.reshape(shape), tracer_end.reshape(shape)


def solution(mesh):
    sizes = (mesh.shape["lat"], mesh.shape["lon"], mesh.shape["lev"])
    spec = P(("unit", "lat"), "lon", "lev", None)
    return jax.shard_map(
        functools.partial(on_device, sizes),
        mesh=mesh,
        in_specs=(spec, spec, spec),
        out_specs=(spec, spec),
        check_vma=False,
    )
```

```python
import functools

import jax
import jax.numpy as jnp
from jax import lax
from jax.experimental import pallas as pl
from jax.experimental.pallas import tpu as pltpu
from jax.sharding import PartitionSpec as P

STEPS = 4
PAD = 8
EPSILON = 0.0001
MESH = pl.DeviceIdType.MESH


def rows_of(extent):
    for rows in (32, 16, 8):
        if extent % rows == 0:
            return rows
    return extent


def steps_kernel(
    sizes, shape, tracer, diffusivity, source, standardized, tracer_end,
    field, coeff, forcing, last, own, others,
    load_sem, lev_send, lev_recv, lat_send, lat_recv, lon_send, lon_recv, stat_send, stat_recv,
):
    n_j, n_i, n_k, _ = shape
    n_lat, n_lon, n_lev = sizes
    inner = pl.ds(PAD, n_i)
    whole_j = pl.ds(1, n_j)
    chunk = rows_of(n_i)
    lat, lon, lev = lax.axis_index("lat"), lax.axis_index("lon"), lax.axis_index("lev")
    lat_up, lat_down = lax.rem(lat + 1, n_lat), lax.rem(lat + n_lat - 1, n_lat)
    lon_up, lon_down = lax.rem(lon + 1, n_lon), lax.rem(lon + n_lon - 1, n_lon)
    lev_up, lev_down = lax.rem(lev + 1, n_lev), lax.rem(lev + n_lev - 1, n_lev)

    def load(which, k):
        array = (tracer, diffusivity, source)[which]
        if which == 0:
            target = field.at[0, k + 1, whole_j, inner, :]
        else:
            target = (coeff, forcing)[which - 1].at[k]
        return pltpu.make_async_copy(array.at[:, :, k, :], target, load_sem.at[which, k])

    def remote(src, dst, send, recv, device):
        return pltpu.make_async_remote_copy(
            src_ref=src, dst_ref=dst, send_sem=send, recv_sem=recv,
            device_id=device, device_id_type=MESH,
        )

    def lev_copies(step, j):
        down = remote(
            field.at[step, 1, j, inner, :], field.at[step, n_k + 1, j, inner, :],
            lev_send.at[step, j - 1, 0], lev_recv.at[step, j - 1, 0], {"lev": lev_down},
        )
        up = remote(
            field.at[step, n_k, j, inner, :], field.at[step, 0, j, inner, :],
            lev_send.at[step, j - 1, 1], lev_recv.at[step, j - 1, 1], {"lev": lev_up},
        )
        return down, up

    parts = (pl.ds(1, 1), pl.ds(n_k, 1), pl.ds(2, n_k - 2))

    def lat_copy(step, part, side):
        k = parts[part]
        src, dst, to = ((1, n_j + 1, lat_down), (n_j, 0, lat_up))[side]
        return remote(
            field.at[step, k, src, inner, :], field.at[step, k, dst, inner, :],
            lat_send.at[step, part, side], lat_recv.at[step, part, side], {"lat": to},
        )

    def lon_copy(step, part, side):
        k = parts[part]
        src, dst, to = (
            (PAD, PAD + n_i, lon_down), (PAD + n_i - 1, PAD - 1, lon_up)
        )[side]
        return remote(
            field.at[step, k, whole_j, pl.ds(src, 1), :],
            field.at[step, k, whole_j, pl.ds(dst, 1), :],
            lon_send.at[step, part, side], lon_recv.at[step, part, side], {"lon": to},
        )

    def stat_copies(j):
        return [
            remote(
                own.at[j - 1], others.at[n_lev - 1 - away, j - 1],
                stat_send.at[away - 1, j - 1], stat_recv.at[n_lev - 1 - away, j - 1],
                {"lev": lax.rem(lev + away, n_lev)},
            )
            for away in range(1, n_lev)
        ]

    def update(step, k, j):
        for low in range(0, n_i, chunk):
            r = PAD + low
            middle = field[step, k, j, pl.ds(r, chunk), :]
            spread = (
                field[step, k, j - 1, pl.ds(r, chunk), :] + field[step, k, j + 1, pl.ds(r, chunk), :]
                + field[step, k, j, pl.ds(r - 1, chunk), :] + field[step, k, j, pl.ds(r + 1, chunk), :]
                + field[step, k - 1, j, pl.ds(r, chunk), :] + field[step, k + 1, j, pl.ds(r, chunk), :]
                - 6.0 * middle
            )
            rows = pl.ds(low, chunk)
            value = middle + coeff[k - 1, j - 1, rows, :] * spread + forcing[k - 1, j - 1, rows, :]
            if step == STEPS - 1:
                last[k - 1, j - 1, rows, :] = value
                place = pl.ds(low * n_k + k - 1, chunk, stride=n_k)
                tracer_end[j - 1, place, :] = value
            else:
                field[step + 1, k, j, pl.ds(r, chunk), :] = value

    def summarise(j):
        for low in range(0, n_i, chunk):
            rows = pl.ds(low, chunk)
            total = last[0, j - 1, rows, :]
            for k in range(1, n_k):
                total = total + last[k, j - 1, rows, :]
            mean = total * (1.0 / n_k)
            squares = jnp.zeros_like(mean)
            for k in range(n_k):
                moved = last[k, j - 1, rows, :] - mean
                squares = squares + moved * moved
            own[j - 1, 0, rows, :] = mean
            own[j - 1, 1, rows, :] = squares

    def combine(j):
        for low in range(0, n_i, chunk):
            rows = pl.ds(low, chunk)
            means = [own[j - 1, 0, rows, :]] + [others[p, j - 1, 0, rows, :] for p in range(n_lev - 1)]
            mean = functools.reduce(jnp.add, means) * (1.0 / n_lev)
            squares = own[j - 1, 1, rows, :]
            for p in range(n_lev - 1):
                squares = squares + others[p, j - 1, 1, rows, :]
            for part in means:
                squares = squares + n_k * ((part - mean) * (part - mean))
            scale = lax.rsqrt(squares * (1.0 / (n_k * n_lev)) + EPSILON)
            for k in range(n_k):
                place = pl.ds(low * n_k + k, chunk, stride=n_k)
                standardized[j - 1, place, :] = (last[k, j - 1, rows, :] - mean) * scale

    def over_k(first, end, body):
        def wrapped(k, carry):
            body(k)
            return carry
        lax.fori_loop(first, end, wrapped, 0)

    edges = (0, n_k - 1)
    for k in (0, n_k - 1, 1, n_k - 2):
        load(0, k).start()
    for which in (1, 2):
        for k in edges:
            load(which, k).start()
    over_k(2, n_k - 2, lambda k: load(0, k).start())
    for which in (1, 2):
        over_k(1, n_k - 1, lambda k: load(which, k).start())

    barrier = pltpu.get_barrier_semaphore()
    greeted = (
        [{"lat": lax.rem(lat + a, n_lat)} for a in sorted({1, n_lat - 1})]
        + [{"lon": lax.rem(lon + a, n_lon)} for a in sorted({1, n_lon - 1})]
        + [{"lev": lax.rem(lev + a, n_lev)} for a in range(1, n_lev)]
    )
    for device in greeted:
        pl.semaphore_signal(barrier, inc=1, device_id=device, device_id_type=MESH)
    pl.semaphore_wait(barrier, len(greeted))

    for k in edges:
        load(0, k).wait()
    for j in range(1, n_j + 1):
        for copy in lev_copies(0, j):
            copy.start()
    for part in (0, 1):
        for side in (0, 1):
            lat_copy(0, part, side).start()
            lon_copy(0, part, side).start()
    for k in (1, n_k - 2):
        load(0, k).wait()
    for which in (1, 2):
        for k in edges:
            load(which, k).wait()

    def inside(step):
        for side in (0, 1):
            lat_copy(step, 2, side).wait_recv()
            lon_copy(step, 2, side).wait_recv()

        def body(k):
            def across(j, carry):
                update(step, k, j)
                return carry
            lax.fori_loop(1, n_j + 1, across, 0)

        over_k(2, n_k, body)
        if step < STEPS - 1:
            for side in (0, 1):
                lat_copy(step + 1, 2, side).start()
                lon_copy(step + 1, 2, side).start()

    def outside(step):
        for part in (0, 1):
            for side in (0, 1):
                lat_copy(step, part, side).wait_recv()
                lon_copy(step, part, side).wait_recv()
        for j in range(1, n_j + 1):
            for copy in lev_copies(step, j):
                copy.wait_recv()
            update(step, 1, j)
            update(step, n_k, j)
            if step < STEPS - 1:
                for copy in lev_copies(step + 1, j):
                    copy.start()
                for side, edge in ((0, 1), (1, n_j)):
                    if j == edge:
                        for part in (0, 1):
                            lat_copy(step + 1, part, side).start()
            else:
                summarise(j)
                for copy in stat_copies(j):
                    copy.start()
        if step < STEPS - 1:
            for part in (0, 1):
                for side in (0, 1):
                    lon_copy(step + 1, part, side).start()

    over_k(2, n_k - 2, lambda k: load(0, k).wait())
    for side in (0, 1):
        lat_copy(0, 2, side).start()
        lon_copy(0, 2, side).start()
    outside(0)
    for which in (1, 2):
        over_k(1, n_k - 1, lambda k: load(which, k).wait())
    inside(0)
    for step in range(1, STEPS):
        inside(step)
        outside(step)
    for j in range(1, n_j + 1):
        for copy in stat_copies(j):
            copy.wait_recv()
        combine(j)

    for step in range(STEPS):
        for j in range(1, n_j + 1):
            for copy in lev_copies(step, j):
                copy.wait_send()
        for part in range(3):
            for side in (0, 1):
                lat_copy(step, part, side).wait_send()
                lon_copy(step, part, side).wait_send()
    for j in range(1, n_j + 1):
        for copy in stat_copies(j):
            copy.wait_send()


def write_kernel(first, second, first_out, second_out, sem):
    copies = [
        pltpu.make_async_copy(src.at[j], dst.at[j], sem.at[which, j])
        for j in range(first.shape[0])
        for which, (src, dst) in enumerate(((first, first_out), (second, second_out)))
    ]
    for copy in copies:
        copy.start()
    for copy in copies:
        copy.wait()


def on_device(sizes, tracer, diffusivity, source):
    shape = tracer.shape
    n_j, n_i, n_k, levels = shape
    n_lev = sizes[2]
    f32 = jnp.float32
    sem = pltpu.SemaphoreType.DMA
    standardized, tracer_end = pl.pallas_call(
        functools.partial(steps_kernel, sizes, shape),
        out_shape=(
            pltpu.VMEM((n_j, n_i * n_k, levels), f32),
            pltpu.VMEM((n_j, n_i * n_k, levels), f32),
        ),
        in_specs=[pl.BlockSpec(memory_space=pl.ANY)] * 3,
        out_specs=(pl.BlockSpec(memory_space=pltpu.VMEM),) * 2,
        scratch_shapes=[
            pltpu.VMEM((STEPS, n_k + 2, n_j + 2, n_i + 2 * PAD, levels), f32),
            pltpu.VMEM((n_k, n_j, n_i, levels), f32),
            pltpu.VMEM((n_k, n_j, n_i, levels), f32),
            pltpu.VMEM((n_k, n_j, n_i, levels), f32),
            pltpu.VMEM((n_j, 2, n_i, levels), f32),
            pltpu.VMEM((n_lev - 1, n_j, 2, n_i, levels), f32),
            sem((3, n_k)),
            sem((STEPS, n_j, 2)), sem((STEPS, n_j, 2)),
            sem((STEPS, 3, 2)), sem((STEPS, 3, 2)),
            sem((STEPS, 3, 2)), sem((STEPS, 3, 2)),
            sem((n_lev - 1, n_j)), sem((n_lev - 1, n_j)),
        ],
        compiler_params=pltpu.CompilerParams(
            collective_id=0, has_side_effects=True, vmem_limit_bytes=48 * 1024 * 1024,
        ),
    )(tracer, diffusivity, source)
    flat = jax.ShapeDtypeStruct((n_j, n_i * n_k, levels), f32)
    standardized, tracer_end = pl.pallas_call(
        write_kernel,
        out_shape=(flat, flat),
        in_specs=[pl.BlockSpec(memory_space=pltpu.VMEM)] * 2,
        out_specs=(pl.BlockSpec(memory_space=pl.ANY),) * 2,
        scratch_shapes=[sem((2, n_j))],
        compiler_params=pltpu.CompilerParams(vmem_limit_bytes=1024 * 1024),
    )(standardized, tracer_end)
    return standardized.reshape(shape), tracer_end.reshape(shape)


def solution(mesh):
    sizes = (mesh.shape["lat"], mesh.shape["lon"], mesh.shape["lev"])
    spec = P(("unit", "lat"), "lon", "lev", None)
    return jax.shard_map(
        functools.partial(on_device, sizes),
        mesh=mesh,
        in_specs=(spec, spec, spec),
        out_specs=(spec, spec),
        check_vma=False,
    )
```
